32 devices in a mesh: pp: 8 (over z, y), ep: 4 (over x, core).
Axes of the slice: x: 2, y: 2, z: 4, core: 2. Of those that a mesh axis runs over, the one named last changes fastest.
Arguments:
- expert_out: bfloat16 [8, 64, 160, 3584], P('pp', 'ep')
- expert_ids: int32 [8, 4, 256, 8], P('pp', 'ep')
- slot_ids: int32 [8, 4, 256, 8], P('pp', 'ep')
- gate_vals: float32 [8, 4, 256, 8], P('pp', 'ep')
- residual: bfloat16 [8, 4, 256, 3584], P('pp', 'ep')
- norm_w: float32 [8, 3584], P('pp')
- w_query: bfloat16 [8, 3584, 28, 128], P('pp')
- w_key: bfloat16 [8, 3584, 28, 128], P('pp')
- w_value: bfloat16 [8, 3584, 28, 128], P('pp')
- w_out: bfloat16 [8, 28, 128, 3584], P('pp')
Outputs:
- output: bfloat16 [8, 4, 256, 3584], P('pp', 'ep')
All inputs are finite; a program needn't handle non-finite values.
Results may differ from the reference program's by a relative error of at most 0.0131893.
Values are sent between devices in bfloat16 or wider.
A program may use at most 1 GiB of HBM per device.

```python
import jax
import jax.numpy as jnp
from jax import lax

STAGES = 8
GROUP_SIZE = 4
NUM_MICRO = 1
SEQ_LEN = 256
SEQS_PER_DEV = 1
D_MODEL = 3584
NUM_EXPERTS = 64
TOP_K = 8
NUM_HEADS = 28
HEAD_DIM = 128
SRC_SLOTS = 40

TOKENS_DEV = SEQS_PER_DEV * SEQ_LEN
SEQS_ALL = GROUP_SIZE * SEQS_PER_DEV
CAPACITY = GROUP_SIZE * SRC_SLOTS
NUM_ROWS = STAGES * NUM_MICRO
QKV_WIDTH = NUM_HEADS * HEAD_DIM
NORM_EPS = 1e-6


def block_ranks(block_ids):
    perm_order = jnp.argsort(block_ids, stable=True)
    sorted_ids = block_ids[perm_order]
    group_start = jnp.searchsorted(sorted_ids, sorted_ids, side='left')
    rank_sorted = jnp.arange(block_ids.shape[0]) - group_start
    return jnp.zeros_like(block_ids).at[perm_order].set(rank_sorted)


def draw_routing(route_key):
    key_bias, key_hot, key_shift, key_noise, key_order = jax.random.split(route_key, 5)
    expert_bias = jnp.sum(jax.random.randint(key_bias, (NUM_ROWS, NUM_EXPERTS, 4), 0, 166, jnp.int32), axis=-1)
    hot_expert = jax.random.randint(key_hot, (NUM_ROWS,), 0, NUM_EXPERTS)
    cover_shift = jax.random.randint(key_shift, (NUM_ROWS,), 0, NUM_EXPERTS)
    local_pos = jnp.arange(TOKENS_DEV)
    expert_pos = jnp.arange(NUM_EXPERTS)
    tie_break = (NUM_EXPERTS - 1 - expert_pos).astype(jnp.int32)

    def one_block(flat_idx):
        row_idx = flat_idx // GROUP_SIZE
        blk_idx = flat_idx % GROUP_SIZE
        noise_draws = jnp.sum(jax.random.randint(jax.random.fold_in(key_noise, flat_idx), (TOKENS_DEV, NUM_EXPERTS, 3), 0, 164, jnp.int32), axis=-1)
        token_pos = blk_idx * TOKENS_DEV + local_pos
        is_cover = (token_pos[:, None] + cover_shift[row_idx]) % NUM_EXPERTS == expert_pos[None, :]
        is_hot = expert_pos[None, :] == hot_expert[row_idx]
        score_int = (expert_bias[row_idx][None, :] + noise_draws) * NUM_EXPERTS + tie_break[None, :] + (1 << 22) * is_cover.astype(jnp.int32) + (1 << 23) * is_hot.astype(jnp.int32)
        chosen = lax.top_k(score_int, TOP_K)[1]
        order_bits = jax.random.bits(jax.random.fold_in(key_order, flat_idx), (TOKENS_DEV, TOP_K), jnp.uint32) >> 8
        order_key = order_bits * TOP_K + jnp.arange(TOP_K, dtype=jnp.uint32)[None, :]
        perm_order = jnp.argsort(order_key, axis=1)
        chosen = jnp.take_along_axis(chosen, perm_order, axis=1)
        slot_rank = block_ranks(chosen.reshape(TOKENS_DEV * TOP_K)).reshape(TOKENS_DEV, TOP_K)
        slot_ids = jnp.where(slot_rank < SRC_SLOTS, blk_idx * SRC_SLOTS + slot_rank, -1)
        return chosen.astype(jnp.int32), slot_ids.astype(jnp.int32)

    expert_ids, slot_ids = lax.map(one_block, jnp.arange(NUM_ROWS * GROUP_SIZE))
    route_shape = (NUM_ROWS, SEQS_ALL, SEQ_LEN, TOP_K)
    return expert_ids.reshape(route_shape), slot_ids.reshape(route_shape)


def draw_bf16(draw_key, arr_shape, scale_fac):
    def one_slice(slice_key):
        return (scale_fac * jax.random.normal(slice_key, arr_shape[1:], jnp.float32)).astype(jnp.bfloat16)
    return lax.map(one_slice, jax.random.split(draw_key, arr_shape[0]))


def setup_inputs(seed: int = 0) -> dict:
    root_key = jax.random.key(seed)
    sub_keys = jax.random.split(root_key, 10)
    expert_ids, slot_ids = draw_routing(sub_keys[0])
    gate_vals = jax.nn.softmax(1.5 * jax.random.normal(sub_keys[1], (NUM_ROWS, SEQS_ALL, SEQ_LEN, TOP_K), jnp.float32), axis=-1)
    expert_scale = 1.5 * jnp.exp(0.5 * jax.random.normal(sub_keys[2], (NUM_ROWS * NUM_EXPERTS,), jnp.float32))

    def expert_slab(slab_args):
        slab_key, slab_scale = slab_args
        return (slab_scale * jax.random.normal(slab_key, (CAPACITY, D_MODEL), jnp.float32)).astype(jnp.bfloat16)

    expert_out = lax.map(expert_slab, (jax.random.split(sub_keys[3], NUM_ROWS * NUM_EXPERTS), expert_scale))
    expert_out = expert_out.reshape(NUM_ROWS, NUM_EXPERTS, CAPACITY, D_MODEL)
    residual = draw_bf16(sub_keys[4], (NUM_ROWS * SEQS_ALL, SEQ_LEN, D_MODEL), 1.0)
    residual = residual.reshape(NUM_ROWS, SEQS_ALL, SEQ_LEN, D_MODEL)
    norm_w = 1.0 + 0.4 * jax.random.normal(sub_keys[5], (STAGES, D_MODEL), jnp.float32)
    in_scale = D_MODEL ** -0.5
    out_scale = QKV_WIDTH ** -0.5
    w_query = draw_bf16(sub_keys[6], (STAGES, D_MODEL, NUM_HEADS, HEAD_DIM), 1.5 * in_scale)
    w_key = draw_bf16(sub_keys[7], (STAGES, D_MODEL, NUM_HEADS, HEAD_DIM), 1.5 * in_scale)
    w_value = draw_bf16(sub_keys[8], (STAGES, D_MODEL, NUM_HEADS, HEAD_DIM), in_scale)
    w_out = draw_bf16(sub_keys[9], (STAGES, NUM_HEADS, HEAD_DIM, D_MODEL), out_scale)
    return dict(expert_out=expert_out, expert_ids=expert_ids, slot_ids=slot_ids, gate_vals=gate_vals, residual=residual, norm_w=norm_w, w_query=w_query, w_key=w_key, w_value=w_value, w_out=w_out)


def reference(expert_out, expert_ids, slot_ids, gate_vals, residual, norm_w, w_query, w_key, w_value, w_out):
    causal = jnp.arange(SEQ_LEN)[:, None] >= jnp.arange(SEQ_LEN)[None, :]

    def one_stage(stage_idx):
        src_stage = (stage_idx + STAGES - 1) % STAGES
        stage_norm = norm_w[stage_idx]
        stage_wq = w_query[stage_idx].reshape(D_MODEL, QKV_WIDTH)
        stage_wk = w_key[stage_idx].reshape(D_MODEL, QKV_WIDTH)
        stage_wv = w_value[stage_idx].reshape(D_MODEL, QKV_WIDTH)
        stage_wo = w_out[stage_idx].reshape(QKV_WIDTH, D_MODEL)

        def project(x_in, weight_mat):
            head_out = jnp.dot(x_in, weight_mat, preferred_element_type=jnp.float32).astype(jnp.bfloat16)
            return head_out.reshape(SEQ_LEN, NUM_HEADS, HEAD_DIM).astype(jnp.float32)

        def one_sequence(flat_idx):
            src_row = src_stage * NUM_MICRO + flat_idx // SEQS_ALL
            seq_idx = flat_idx % SEQS_ALL
            ids_seq = expert_ids[src_row, seq_idx]
            slot_seq = slot_ids[src_row, seq_idx]
            is_kept = slot_seq >= 0
            picked = expert_out[src_row, ids_seq, jnp.where(is_kept, slot_seq, 0)].astype(jnp.float32)
            weight = jnp.where(is_kept, gate_vals[src_row, seq_idx], 0.0)
            mixed_sum = residual[src_row, seq_idx].astype(jnp.float32) + jnp.sum(weight[:, :, None] * picked, axis=1)
            y_wide = mixed_sum.astype(jnp.bfloat16).astype(jnp.float32)
            inv_rms = lax.rsqrt(jnp.mean(y_wide * y_wide, axis=-1, keepdims=True) + NORM_EPS)
            x_in = (y_wide * inv_rms * stage_norm).astype(jnp.bfloat16)
            q_heads = project(x_in, stage_wq)
            k_heads = project(x_in, stage_wk)
            v_heads = project(x_in, stage_wv)
            scores = jnp.einsum('qhe,khe->hqk', q_heads, k_heads) * HEAD_DIM ** -0.5
            attn_probs = jax.nn.softmax(jnp.where(causal, scores, -jnp.inf), axis=-1).astype(jnp.bfloat16)
            attn_out = jnp.einsum('hqk,khe->qhe', attn_probs.astype(jnp.float32), v_heads).astype(jnp.bfloat16)
            out_proj = jnp.dot(attn_out.reshape(SEQ_LEN, QKV_WIDTH), stage_wo, preferred_element_type=jnp.float32).astype(jnp.bfloat16)
            return (y_wide + out_proj.astype(jnp.float32)).astype(jnp.bfloat16)

        return lax.map(one_sequence, jnp.arange(NUM_MICRO * SEQS_ALL))

    stage_outs = lax.map(one_stage, jnp.arange(STAGES))
    return stage_outs.reshape(NUM_ROWS, SEQS_ALL, SEQ_LEN, D_MODEL)
```

```python
import functools

import jax
import jax.numpy as jnp
from jax import lax
from jax.experimental import pallas as pl
from jax.experimental.pallas import tpu as pltpu
from jax.sharding import PartitionSpec as P

NORM_EPS = 1e-6
MESH = pl.DeviceIdType.MESH
BF16 = jnp.bfloat16
F32 = jnp.float32


def fused_kernel(stages, o_ref, idx_ref, slot_ref, gate_ref, h_ref, nw_ref, wq_ref, wk_ref, wv_ref, wo_ref, z_ref,
                 obx, obo, rtab_i, rtab_s, rtab_g, gx, go, snd, rcv, hbuf, yb, xb, qb, kb, vb, ab, wb, zb,
                 tab_s, tab_r, h_sem, loc_x, loc_o, dx_s, dx_r, do_s, do_r, x_s, x_r, y_s, y_r, r_s, r_r,
                 a_s, a_r, z_l, z_s, z_r, w_sem):
    n_chunk, _, src, width = obx.shape
    n_exp, cap, d_model = o_ref.shape
    n_rows = 2 * n_exp * src
    tokens = h_ref.shape[0]
    part = tokens // 2
    n_pick = idx_ref.shape[0]
    n_pair = kb.shape[1]
    head_dim = wq_ref.shape[2]
    scale = head_dim ** -0.5
    stage = lax.axis_index('pp')
    me = lax.axis_index('ep')
    chip = me // 2
    core = me % 2
    sib = chip * 2 + (1 - core)
    peer = (1 - chip) * 2 + core
    sib_peer = (1 - chip) * 2 + (1 - core)
    to_sib = {'pp': stage, 'ep': sib}
    to_peer = {'pp': stage, 'ep': peer}
    to_next = {'pp': (stage + 1) % stages, 'ep': me}
    to_prev = {'pp': (stage + stages - 1) % stages, 'ep': me}

    def remote(a, b, send, recv, dev):
        return pltpu.make_async_remote_copy(a, b, send, recv, device_id=dev, device_id_type=MESH)

    def rows_of(owner, k):
        return o_ref.at[:, pl.ds(pl.multiple_of(owner * src, 8), src), pl.ds(pl.multiple_of(k * width, width), width)]

    def half_of(buf, k, core_idx):
        return buf.at[k, pl.ds(core_idx * n_exp, n_exp)]

    def load_pair(i, s):
        for m, w in enumerate((wq_ref, wk_ref, wv_ref)):
            for t in range(2):
                pltpu.make_async_copy(
                    w.at[core * (2 * n_pair) + 2 * i + t],
                    wb.at[s, :, pl.ds(m * width + t * head_dim, head_dim)], w_sem.at[s, m]).start()

    def load_tile(n):
        s, m = tile_slot(n)
        pltpu.make_async_copy(
            wo_ref.at[:, pl.ds(pl.multiple_of((core * n_pair + n) * width, width), width)],
            wb.at[s, :, pl.ds(m * width, width)], w_sem.at[s, m]).start()

    def tile_slot(n):
        return (1, n) if n < 3 else (0, n - 3) if n < 6 else (1, 0)

    def wait_tile(s, m):
        dst = wb.at[s, :, pl.ds(m * width, width)]
        pltpu.make_async_copy(dst, dst, w_sem.at[s, m]).wait()

    barrier = pltpu.get_barrier_semaphore()
    for dev in (to_sib, to_peer, to_next, to_prev):
        pl.semaphore_signal(barrier, inc=1, device_id=dev, device_id_type=MESH)

    @pl.loop(0, n_chunk)
    def _(k):
        pltpu.make_async_copy(rows_of(peer, k), half_of(obx, k, core), loc_x.at[k]).start()

    def build(idx, slot, gate, owner, out, halves):
        first = chip * (2 * n_exp)
        keep = (slot >= 0) & (idx >= first) & (idx < first + 2 * n_exp)
        key = jnp.where(keep, (idx - first) * src + (slot - owner * src), -1)
        key_t = key.T
        gate_t = gate.T
        rows = 64
        for hf in halves:
            for low in range(0, part, rows):
                kr = key_t[hf * part + low:hf * part + low + rows]
                gr = gate_t[hf * part + low:hf * part + low + rows]
                for b in range(n_rows // 128):
                    lane = lax.broadcasted_iota(jnp.int32, (rows, 128), 1) + b * 128
                    acc = jnp.zeros((rows, 128), F32)
                    for i in range(n_pick):
                        acc = jnp.where(kr[:, i:i + 1] == lane, gr[:, i:i + 1], acc)
                    for t in range(3):
                        top = acc.astype(BF16)
                        out[hf, t * part + low:t * part + low + rows, b * 128:(b + 1) * 128] = top
                        acc = acc - top.astype(F32)

    def mix(table, rows):
        full = jnp.dot(table, rows, preferred_element_type=F32)
        return (full[2 * part:] + full[part:2 * part]) + full[:part]

    def wait_rows(buf, loc, send, recv, k):
        mine = half_of(buf, k, core)
        pltpu.make_async_copy(mine, mine, loc.at[k]).wait()
        other = half_of(buf, k, 1 - core)
        remote(other, other, send.at[k], recv.at[k], to_sib).wait_recv()

    def send_part(g):
        return remote(snd.at[g], rcv.at[g], x_s.at[g], x_r.at[g], to_peer)

    def y_slot(g):
        return yb.at[g, pl.ds(pl.multiple_of(core * part, 8), part)]

    def send_y(g):
        return remote(hbuf.at[g], y_slot(g), y_s.at[g], y_r.at[g], to_next)

    def relay_copy(g):
        return remote(y_slot(g), y_slot(g), r_s.at[g], r_r.at[g], to_sib)

    def chunk(g, hf, k):
        mine = mix(go[hf], obo[k].reshape(n_rows, width))
        send_part(g).wait_recv()
        hbuf[g] = (hbuf[g].astype(F32) + (mine + rcv[g])).astype(BF16)
        send_y(g).start()

    def relay(g):
        send_y(g).wait_recv()
        relay_copy(g).start()

    def prepare(hf):
        @pl.loop(hf * n_chunk, (hf + 1) * n_chunk)
        def _(g):
            other = yb.at[g, pl.ds(pl.multiple_of((1 - core) * part, 8), part)]
            remote(other, other, r_s.at[g], r_r.at[g], to_sib).wait_recv()
        total = jnp.zeros((tokens, width), F32)
        for k in range(n_chunk):
            y = yb[hf * n_chunk + k].astype(F32)
            total = total + y * y
        inv = lax.rsqrt(jnp.sum(total, axis=-1, keepdims=True) * (1.0 / d_model) + NORM_EPS)
        for k in range(n_chunk):
            y = yb[hf * n_chunk + k].astype(F32)
            cols = slice(k * width, (k + 1) * width)
            xb[:, cols] = (y * inv * nw_ref[:, cols]).astype(BF16)

    def send_heads(hf, i):
        cols = pl.ds(pl.multiple_of((core * n_pair + i) * width, width), width)
        return remote(ab.at[hf, :, cols], ab.at[hf, :, cols], a_s.at[hf * n_pair + i], a_r.at[hf * n_pair + i], to_sib)

    def wait_set(s):
        for m in range(3):
            wait_tile(s, m)

    def attend(hf, i):
        keys = (hf + 1) * part
        row = lax.broadcasted_iota(jnp.int32, (part, keys), 0) + hf * part
        col = lax.broadcasted_iota(jnp.int32, (part, keys), 1)
        for q in range(2):
            for t in range(2):
                hd = slice(t * head_dim, (t + 1) * head_dim)
                qh = qb[q * part:(q + 1) * part, hd]
                kh = kb[q, i, :keys, hd]
                vh = vb[q, i, :keys, hd]
                sc = lax.dot_general(qh, kh, (((1,), (1,)), ((), ())), preferred_element_type=F32) * scale
                sc = jnp.where(row >= col, sc, -jnp.inf)
                p = jnp.exp(sc - jnp.max(sc, axis=-1, keepdims=True))
                p = (p * (1.0 / jnp.sum(p, axis=-1, keepdims=True))).astype(BF16)
                out = jnp.dot(p, vh, preferred_element_type=F32).astype(BF16)
                ab[hf, q * part:(q + 1) * part,
                   pl.ds(pl.multiple_of((core * n_pair + i) * width + t * head_dim, head_dim), head_dim)] = out

    def heads(hf, i):
        s = i % 2
        x = xb[...]
        out = [jnp.dot(x, wb[s, :, m * width:(m + 1) * width], preferred_element_type=F32).astype(BF16) for m in range(3)]
        qb[...] = out[0]
        for q in range(2):
            kb[q, i, hf * part:(hf + 1) * part, :] = out[1][q * part:(q + 1) * part]
            vb[q, i, hf * part:(hf + 1) * part, :] = out[2][q * part:(q + 1) * part]

    def pair(hf, i):
        wait_set(i % 2)
        attend(hf, i - 1)
        heads(hf, i)
        send_heads(hf, i - 1).start()

        @pl.when(i < n_pair - 2)
        def _():
            load_pair(i + 2, i % 2)

        @pl.when(i == n_pair - 2)
        def _():
            for n in range(3):
                load_tile(n)

        @pl.when(i == n_pair - 1)
        def _():
            for n in range(3, 6):
                load_tile(n)

    def first_pair(hf):
        wait_set(0)
        heads(hf, 0)
        load_pair(2, 0)

    def last_pair(hf):
        attend(hf, n_pair - 1)
        send_heads(hf, n_pair - 1).start()

    def z_copies(hf, n):
        cols = pl.ds(pl.multiple_of((core * n_pair + n) * width, width), width)
        dst = z_ref.at[pl.ds(hf * part, part), cols]
        j = hf * n_pair + n
        keep = zb.at[j, pl.ds(pl.multiple_of(core * part, 8), part)]
        give = zb.at[j, pl.ds(pl.multiple_of((1 - core) * part, 8), part)]
        return pltpu.make_async_copy(keep, dst, z_l.at[j]), remote(give, dst, z_s.at[j], z_r.at[j], to_sib)

    def wait_heads(hf):
        for i in range(n_pair):
            cols = pl.ds(pl.multiple_of(((1 - core) * n_pair + i) * width, width), width)
            dst = ab.at[hf, :, cols]
            j = hf * n_pair + i
            remote(dst, dst, a_s.at[j], a_r.at[j], to_sib).wait_recv()

    def project(hf, tiles):
        for n in tiles:
            wait_tile(*tile_slot(n))
        for n in tiles:
            s, m = tile_slot(n)
            out = jnp.dot(ab[hf], wb[s, :, m * width:(m + 1) * width], preferred_element_type=F32).astype(BF16)
            y = yb[hf * n_chunk + core * n_pair + n].astype(F32)
            zb[hf * n_pair + n] = (y + out.astype(F32)).astype(BF16)
        for n in tiles:
            for c in z_copies(hf, n):
                c.start()
            if n == 0:
                load_tile(6)
            if hf == 0 and n == 5:
                load_pair(0, 0)
            if hf == 0 and n == 6:
                load_pair(1, 1)

    build(idx_ref[...], slot_ref[...], gate_ref[...], me, go, (0,))
    pl.semaphore_wait(barrier, 4)

    tabs = [remote(a, b, tab_s.at[i], tab_r.at[i], to_peer)
            for i, (a, b) in enumerate(((idx_ref, rtab_i), (slot_ref, rtab_s), (gate_ref, rtab_g)))]
    for t in tabs:
        t.start()

    @pl.loop(0, n_chunk)
    def _(k):
        remote(rows_of(sib_peer, k), half_of(obx, k, core), dx_s.at[k], dx_r.at[k], to_sib).start()

    for hf in range(2):
        @pl.loop(0, n_chunk)
        def _(k):
            pltpu.make_async_copy(
                h_ref.at[pl.ds(hf * part, part), pl.ds(pl.multiple_of(k * width, width), width)],
                hbuf.at[hf * n_chunk + k], h_sem).start()

    @pl.loop(0, n_chunk)
    def _(k):
        pltpu.make_async_copy(rows_of(me, k), half_of(obo, k, core), loc_o.at[k]).start()
        remote(rows_of(sib, k), half_of(obo, k, core), do_s.at[k], do_r.at[k], to_sib).start()

    for t in tabs:
        t.wait()
    build(rtab_i[...], rtab_s[...], rtab_g[...], peer, gx, (0,))

    @pl.loop(0, n_chunk)
    def _(k):
        wait_rows(obx, loc_x, dx_s, dx_r, k)
        snd[k] = mix(gx[0], obx[k].reshape(n_rows, width))
        send_part(k).start()

    load_pair(0, 0)
    load_pair(1, 1)
    build(rtab_i[...], rtab_s[...], rtab_g[...], peer, gx, (1,))
    build(idx_ref[...], slot_ref[...], gate_ref[...], me, go, (1,))
    pltpu.make_async_copy(hbuf, hbuf, h_sem).wait()

    @pl.loop(0, n_chunk)
    def _(k):
        snd[n_chunk + k] = mix(gx[1], obx[k].reshape(n_rows, width))
        send_part(n_chunk + k).start()
        wait_rows(obo, loc_o, do_s, do_r, k)
        chunk(k, 0, k)

        @pl.when(k >= 2)
        def _():
            relay(k - 2)

    lead = 3

    @pl.loop(0, lead)
    def _(k):
        chunk(n_chunk + k, 1, k)
        relay(n_chunk + k - 2)

    prepare(0)
    first_pair(0)

    @pl.loop(1, n_pair)
    def _(i):
        k = i - 1 + lead
        chunk(n_chunk + k, 1, k)
        relay(n_chunk + k - 2)
        pair(0, i)

    last_pair(0)
    work = {lead + n_pair - 1: None, lead + n_pair: (0, 1, 2), lead + n_pair + 1: (3, 4, 5), lead + n_pair + 2: (6,)}
    for k in range(lead + n_pair - 1, n_chunk):
        chunk(n_chunk + k, 1, k)
        relay(n_chunk + k - 2)
        if k in work:
            if work[k] is None:
                wait_heads(0)
            else:
                project(0, work[k])
    relay(2 * n_chunk - 2)
    relay(2 * n_chunk - 1)
    prepare(1)
    first_pair(1)

    @pl.loop(1, n_pair)
    def _(i):
        pair(1, i)

    last_pair(1)
    wait_heads(1)
    project(1, (0, 1, 2))
    project(1, (3, 4, 5))
    project(1, (6,))

    @pl.loop(0, n_chunk)
    def _(k):
        for buf, s, r in ((obx, dx_s, dx_r), (obo, do_s, do_r)):
            mine = half_of(buf, k, core)
            remote(mine, mine, s.at[k], r.at[k], to_sib).wait_send()

    @pl.loop(0, 2 * n_chunk)
    def _(g):
        send_part(g).wait_send()
        send_y(g).wait_send()
        relay_copy(g).wait_send()

    for hf in range(2):
        for n in range(n_pair):
            send_heads(hf, n).wait_send()
            keep, give = z_copies(hf, n)
            keep.wait()
            give.wait()


def fused_block(stages, expert_out, expert_ids, slot_ids, gate_vals, residual, norm_w, w_query, w_key, w_value, w_out):
    n_exp, cap, d_model = expert_out.shape
    tokens = residual.shape[0]
    n_head, _, head_dim = w_query.shape
    width = 2 * head_dim
    n_chunk = d_model // width
    n_pair = n_head // 4
    part = tokens // 2
    n_rows = 2 * n_exp * (cap // 4)
    n_pick = expert_ids.shape[0]
    dma = pltpu.SemaphoreType.DMA
    any_spec = pl.BlockSpec(memory_space=pl.ANY)
    vmem_spec = pl.BlockSpec(memory_space=pltpu.VMEM)
    vm = pltpu.VMEM
    return pl.pallas_call(
        functools.partial(fused_kernel, stages),
        out_shape=jax.ShapeDtypeStruct((tokens, d_model), BF16),
        in_specs=[any_spec, vmem_spec, vmem_spec, vmem_spec, any_spec, vmem_spec] + [any_spec] * 4,
        out_specs=any_spec,
        scratch_shapes=[
            vm((n_chunk, 2 * n_exp, cap // 4, width), BF16),
            vm((n_chunk, 2 * n_exp, cap // 4, width), BF16),
            vm((n_pick, tokens), jnp.int32),
            vm((n_pick, tokens), jnp.int32),
            vm((n_pick, tokens), F32),
            vm((2, 3 * part, n_rows), BF16),
            vm((2, 3 * part, n_rows), BF16),
            vm((2 * n_chunk, part, width), F32),
            vm((2 * n_chunk, part, width), F32),
            vm((2 * n_chunk, part, width), BF16),
            vm((2 * n_chunk, tokens, width), BF16),
            vm((tokens, d_model), BF16),
            vm((tokens, width), BF16),
            vm((2, n_pair, tokens, width), BF16),
            vm((2, n_pair, tokens, width), BF16),
            vm((2, tokens, d_model), BF16),
            vm((2, d_model, 3 * width), BF16),
            vm((2 * n_pair, tokens, width), BF16),
            dma((3,)), dma((3,)), dma,
        ] + [dma((n_chunk,))] * 6 + [dma((2 * n_chunk,))] * 6 + [dma((2 * n_pair,))] * 5 + [dma((2, 3))],
        compiler_params=pltpu.CompilerParams(collective_id=0, has_side_effects=True, vmem_limit_bytes=67_000_000),
        name='fused_block',
    )(expert_out, expert_ids, slot_ids, gate_vals, residual, norm_w, w_query, w_key, w_value, w_out)


def solution(mesh):
    stages = mesh.shape['pp']
    tok_spec = P('pp', 'ep', None, None)
    wt_spec = P('pp', None, None, None)

    def device_step(expert_out, expert_ids, slot_ids, gate_vals, residual, norm_w, w_query, w_key, w_value, w_out):
        heads = [w[0].transpose(1, 0, 2) for w in (w_query, w_key, w_value)]
        proj = w_out[0].reshape(-1, w_out.shape[3])
        result = fused_block(stages, expert_out[0], expert_ids[0, 0].T, slot_ids[0, 0].T, gate_vals[0, 0].T,
                             residual[0, 0], norm_w, *heads, proj)
        return result.reshape(residual.shape)

    return jax.shard_map(device_step, mesh=mesh, in_specs=(tok_spec, tok_spec, tok_spec, tok_spec, tok_spec, P('pp', None), wt_spec, wt_spec, wt_spec, wt_spec), out_specs=tok_spec, check_vma=False)
```

```python
import functools

import jax
import jax.numpy as jnp
from jax import lax
from jax.experimental import pallas as pl
from jax.experimental.pallas import tpu as pltpu
from jax.sharding import PartitionSpec as P

NORM_EPS = 1e-6
MESH = pl.DeviceIdType.MESH
BF16 = jnp.bfloat16
F32 = jnp.float32


PARTS = (4, 4)
SCHEDULE = (2, 2, (1, 1))


def fused_kernel(stages, o_ref, idx_ref, slot_ref, gate_ref, h_ref, nw_ref, wq_ref, wk_ref, wv_ref, wo_ref, z_ref,
                 obx, obo, rtab_i, rtab_s, rtab_g, gate_tab, tot, xb, qb, kb, vb, wb,
                 snd0, snd1, rcv0, rcv1, own1, hbuf0, hbuf1, yb0, yb1, ab0, ab1, zbuf,
                 tab_s, tab_r, h_sem, loc_x, loc_o, dx_s, dx_r, do_s, do_r, x_s, x_r, y_s, y_r, r_s, r_r,
                 a_s, a_r, z_l, z_s, z_r, w_sem):
    snd, rcv, own, hbuf = (snd0, snd1), (rcv0, rcv1), (None, own1), (hbuf0, hbuf1)
    yb, ab, zb = (yb0, yb1), (ab0, ab1), (zbuf, zbuf)
    n_chunk, _, src, width = obx.shape
    n_exp, cap, d_model = o_ref.shape
    n_rows = 2 * n_exp * src
    tokens = h_ref.shape[0]
    size = [tokens * p // sum(PARTS) for p in PARTS]
    base = [sum(size[:p]) for p in range(2)]
    n_pick = idx_ref.shape[0]
    n_pair = kb.shape[1]
    head_dim = wq_ref.shape[2]
    scale = head_dim ** -0.5
    stage = lax.axis_index('pp')
    me = lax.axis_index('ep')
    chip = me // 2
    core = me % 2
    sib = chip * 2 + (1 - core)
    peer = (1 - chip) * 2 + core
    sib_peer = (1 - chip) * 2 + (1 - core)
    to_sib = {'pp': stage, 'ep': sib}
    to_peer = {'pp': stage, 'ep': peer}
    to_next = {'pp': (stage + 1) % stages, 'ep': me}
    to_prev = {'pp': (stage + stages - 1) % stages, 'ep': me}

    def remote(a, b, send, recv, dev):
        return pltpu.make_async_remote_copy(a, b, send, recv, device_id=dev, device_id_type=MESH)

    def rows_of(owner, k):
        return o_ref.at[:, pl.ds(pl.multiple_of(owner * src, 8), src), pl.ds(pl.multiple_of(k * width, width), width)]

    def half_of(buf, k, core_idx):
        return buf.at[k, pl.ds(core_idx * n_exp, n_exp)]

    def load_pair(i, s):
        for m, w in enumerate((wq_ref, wk_ref, wv_ref)):
            for t in range(2):
                pltpu.make_async_copy(
                    w.at[core * (2 * n_pair) + 2 * i + t],
                    wb.at[s, :, pl.ds(m * width + t * head_dim, head_dim)], w_sem.at[s, m]).start()

    def tile_slot(p, n):
        return (p + 1 + n // 3) % 3, n % 3

    def load_tile(p, n):
        s, m = tile_slot(p, n)
        pltpu.make_async_copy(
            wo_ref.at[:, pl.ds(pl.multiple_of((core * n_pair + n) * width, width), width)],
            wb.at[s, :, pl.ds(m * width, width)], w_sem.at[s, m]).start()

    def wait_tile(s, m):
        dst = wb.at[s, :, pl.ds(m * width, width)]
        pltpu.make_async_copy(dst, dst, w_sem.at[s, m]).wait()

    def build(idx, slot, gate, owner, out, parts):
        first = chip * (2 * n_exp)
        keep = (slot >= 0) & (idx >= first) & (idx < first + 2 * n_exp)
        key = jnp.where(keep, (idx - first) * src + (slot - owner * src), -1)
        key_t = key.T
        gate_t = gate.T
        rows = 64
        for p in parts:
            for low in range(0, size[p], rows):
                kr = key_t[base[p] + low:base[p] + low + rows]
                gr = gate_t[base[p] + low:base[p] + low + rows]
                for b in range(n_rows // 128):
                    lane = lax.broadcasted_iota(jnp.int32, (rows, 128), 1) + b * 128
                    acc = jnp.zeros((rows, 128), F32)
                    for i in range(n_pick):
                        acc = jnp.where(kr[:, i:i + 1] == lane, gr[:, i:i + 1], acc)
                    for t in range(3):
                        top = acc.astype(BF16)
                        at = 3 * base[p] + t * size[p] + low
                        out[at:at + rows, b * 128:(b + 1) * 128] = top
                        acc = acc - top.astype(F32)

    def mix(table, buf, k, parts):
        low, high = 3 * base[parts[0]], 3 * (base[parts[-1]] + size[parts[-1]])
        full = jnp.dot(table[low:high], buf[k].reshape(n_rows, width), preferred_element_type=F32)
        out = []
        for p in parts:
            n, at = size[p], 3 * base[p] - low
            out.append((full[at + 2 * n:at + 3 * n] + full[at + n:at + 2 * n]) + full[at:at + n])
        return out

    def wait_rows(buf, loc, send, recv, k):
        mine = half_of(buf, k, core)
        pltpu.make_async_copy(mine, mine, loc.at[k]).wait()
        other = half_of(buf, k, 1 - core)
        remote(other, other, send.at[k], recv.at[k], to_sib).wait_recv()

    def send_part(p, k):
        g = p * n_chunk + k
        return remote(snd[p].at[k], rcv[p].at[k], x_s.at[g], x_r.at[g], to_peer)

    def y_slot(p, k, whose):
        return yb[p].at[k, pl.ds(pl.multiple_of(whose * size[p], size[p]), size[p])]

    def send_y(p, k):
        g = p * n_chunk + k
        return remote(hbuf[p].at[k], y_slot(p, k, core), y_s.at[g], y_r.at[g], to_next)

    def relay_copy(p, k):
        g = p * n_chunk + k
        return remote(y_slot(p, k, core), y_slot(p, k, core), r_s.at[g], r_r.at[g], to_sib)

    def chunk(p, k):
        if p == 0:
            wait_rows(obo, loc_o, do_s, do_r, k)
            mine, own[1][k] = mix(gate_tab, obo, k, (0, 1))
        else:
            mine = own[p][k]
        send_part(p, k).wait_recv()
        hbuf[p][k] = (hbuf[p][k].astype(F32) + (mine + rcv[p][k])).astype(BF16)
        send_y(p, k).start()

    def relay(p, k):
        send_y(p, k).wait_recv()
        relay_copy(p, k).start()

    def squares(p, k0, k1):
        @pl.loop(k0, k1)
        def _(k):
            g = p * n_chunk + k
            other = y_slot(p, k, 1 - core)
            remote(other, other, r_s.at[g], r_r.at[g], to_sib).wait_recv()
        n = 2 * size[p]
        total = jnp.zeros((n, width), F32) if k0 == 0 else tot[:n]
        for k in range(k0, k1):
            y = yb[p][k].astype(F32)
            total = total + y * y
        tot[:n] = total

    def normed(p):
        n = 2 * size[p]
        inv = lax.rsqrt(jnp.sum(tot[:n], axis=-1, keepdims=True) * (1.0 / d_model) + NORM_EPS)
        for k in range(n_chunk):
            y = yb[p][k].astype(F32)
            cols = slice(k * width, (k + 1) * width)
            xb[:n, cols] = (y * inv * nw_ref[:, cols]).astype(BF16)

    def send_heads(p, i):
        cols = pl.ds(pl.multiple_of((core * n_pair + i) * width, width), width)
        j = p * n_pair + i
        return remote(ab[p].at[:, cols], ab[p].at[:, cols], a_s.at[j], a_r.at[j], to_sib)

    def wait_heads(p):
        for i in range(n_pair):
            cols = pl.ds(pl.multiple_of(((1 - core) * n_pair + i) * width, width), width)
            dst = ab[p].at[:, cols]
            j = p * n_pair + i
            remote(dst, dst, a_s.at[j], a_r.at[j], to_sib).wait_recv()

    def wait_set(s):
        for m in range(3):
            wait_tile(s, m)

    def attend(p, i):
        n, low = size[p], base[p]
        keys = tokens
        row = lax.broadcasted_iota(jnp.int32, (n, keys), 0) + low
        col = lax.broadcasted_iota(jnp.int32, (n, keys), 1)
        for q in range(2):
            for t in range(2):
                hd = slice(t * head_dim, (t + 1) * head_dim)
                qh = qb[q * n:(q + 1) * n, hd]
                kh = kb[q, i, :keys, hd]
                vh = vb[q, i, :keys, hd]
                sc = lax.dot_general(qh, kh, (((1,), (1,)), ((), ())), preferred_element_type=F32) * scale
                sc = jnp.where(row >= col, sc, -jnp.inf)
                e = jnp.exp(sc - jnp.max(sc, axis=-1, keepdims=True))
                e = (e * (1.0 / jnp.sum(e, axis=-1, keepdims=True))).astype(BF16)
                out = jnp.dot(e, vh, preferred_element_type=F32).astype(BF16)
                ab[p][q * n:(q + 1) * n,
                      pl.ds(pl.multiple_of((core * n_pair + i) * width + t * head_dim, head_dim), head_dim)] = out

    def heads(p, i):
        s = (i + p) % 3
        n, low = size[p], base[p]
        x = xb[:2 * n]
        out = [jnp.dot(x, wb[s, :, m * width:(m + 1) * width], preferred_element_type=F32).astype(BF16) for m in range(3)]
        qb[:2 * n] = out[0]
        for q in range(2):
            kb[q, i, low:low + n, :] = out[1][q * n:(q + 1) * n]
            vb[q, i, low:low + n, :] = out[2][q * n:(q + 1) * n]

    def pair(p, i):
        wait_set((i + p) % 3)
        attend(p, i - 1)
        heads(p, i)
        send_heads(p, i - 1).start()

        @pl.when(i < n_pair - 3)
        def _():
            load_pair(i + 3, (i + p) % 3)

        @pl.when(i == n_pair - 3)
        def _():
            for n in range(3):
                load_tile(p, n)

        @pl.when(i == n_pair - 2)
        def _():
            for n in range(3, 6):
                load_tile(p, n)

        @pl.when(i == n_pair - 1)
        def _():
            load_tile(p, 6)

    def first_pair(p):
        wait_set(p)
        heads(p, 0)
        load_pair(3, p)

    def last_pair(p):
        attend(p, n_pair - 1)
        send_heads(p, n_pair - 1).start()

    def z_copies(p, n):
        cols = pl.ds(pl.multiple_of((core * n_pair + n) * width, width), width)
        dst = z_ref.at[pl.ds(base[p], size[p]), cols]
        j = p * n_pair + n
        keep = zb[p].at[n, pl.ds(pl.multiple_of(core * size[p], size[p]), size[p])]
        give = zb[p].at[n, pl.ds(pl.multiple_of((1 - core) * size[p], size[p]), size[p])]
        return pltpu.make_async_copy(keep, dst, z_l.at[j]), remote(give, dst, z_s.at[j], z_r.at[j], to_sib)

    def half_dot(p, n, whose):
        s, m = tile_slot(p, n)
        cut = pl.ds(pl.multiple_of(whose * (d_model // 2), width), d_model // 2)
        return jnp.dot(ab[p][:, cut], wb[s, cut, m * width:(m + 1) * width], preferred_element_type=F32)

    def project_own(p, tiles):
        for n in tiles:
            wait_tile(*tile_slot(p, n))
        for n in tiles:
            own[1][2 * n], own[1][2 * n + 1] = jnp.split(half_dot(p, n, core), 2)

    def project(p, tiles, early):
        if not early:
            for n in tiles:
                wait_tile(*tile_slot(p, n))
        for n in tiles:
            s, m = tile_slot(p, n)
            if early:
                out = (jnp.concatenate((own[1][2 * n], own[1][2 * n + 1])) + half_dot(p, n, 1 - core)).astype(BF16)
            else:
                out = jnp.dot(ab[p][...], wb[s, :, m * width:(m + 1) * width], preferred_element_type=F32).astype(BF16)
            y = yb[p][core * n_pair + n].astype(F32)
            zb[p][n] = (y + out.astype(F32)).astype(BF16)
        for n in tiles:
            for c in z_copies(p, n):
                c.start()
            if p == 0 and n % 3 == 2:
                load_pair(n // 3, (n // 3 + 1) % 3)
            if p == 0 and n == 6:
                load_pair(2, 0)

    def drain_z(p):
        for n in range(n_pair):
            send_heads(p, n).wait_send()
            keep, give = z_copies(p, n)
            keep.wait()
            give.wait()

    barrier = pltpu.get_barrier_semaphore()
    for dev in (to_sib, to_peer, to_next, to_prev):
        pl.semaphore_signal(barrier, inc=1, device_id=dev, device_id_type=MESH)

    @pl.loop(0, n_chunk)
    def _(k):
        pltpu.make_async_copy(rows_of(peer, k), half_of(obx, k, core), loc_x.at[k]).start()

    pl.semaphore_wait(barrier, 4)

    tabs = [remote(a, b, tab_s.at[i], tab_r.at[i], to_peer)
            for i, (a, b) in enumerate(((idx_ref, rtab_i), (slot_ref, rtab_s), (gate_ref, rtab_g)))]
    for t in tabs:
        t.start()

    @pl.loop(0, n_chunk)
    def _(k):
        remote(rows_of(sib_peer, k), half_of(obx, k, core), dx_s.at[k], dx_r.at[k], to_sib).start()

    for p in range(2):
        @pl.loop(0, n_chunk)
        def _(k):
            pltpu.make_async_copy(
                h_ref.at[pl.ds(base[p], size[p]), pl.ds(pl.multiple_of(k * width, width), width)],
                hbuf[p].at[k], h_sem.at[p]).start()

    @pl.loop(0, n_chunk)
    def _(k):
        pltpu.make_async_copy(rows_of(me, k), half_of(obo, k, core), loc_o.at[k]).start()
        remote(rows_of(sib, k), half_of(obo, k, core), do_s.at[k], do_r.at[k], to_sib).start()

    for t in tabs:
        t.wait()
    build(rtab_i[...], rtab_s[...], rtab_g[...], peer, gate_tab, (0,))
    ahead = 2

    @pl.loop(0, ahead)
    def _(k):
        wait_rows(obx, loc_x, dx_s, dx_r, k)
        snd[0][k], = mix(gate_tab, obx, k, (0,))
        send_part(0, k).start()

    build(rtab_i[...], rtab_s[...], rtab_g[...], peer, gate_tab, (1,))

    @pl.loop(ahead, n_chunk)
    def _(k):
        wait_rows(obx, loc_x, dx_s, dx_r, k)
        snd[0][k], snd[1][k] = mix(gate_tab, obx, k, (0, 1))
        send_part(0, k).start()

    @pl.loop(0, ahead)
    def _(k):
        snd[1][k], = mix(gate_tab, obx, k, (1,))

    for i in range(3):
        load_pair(i, i)
    build(idx_ref[...], slot_ref[...], gate_ref[...], me, gate_tab, (0, 1))
    for p in range(2):
        pltpu.make_async_copy(hbuf[p], hbuf[p], h_sem.at[p]).wait()

    for q in range(2):
        @pl.loop(0, n_pair)
        def _(i):
            kb[q, i, base[1]:, :] = jnp.zeros((size[1], width), BF16)
            vb[q, i, base[1]:, :] = jnp.zeros((size[1], width), BF16)

    @pl.loop(0, n_chunk)
    def _(k):
        send_part(1, k).start()
        chunk(0, k)

        @pl.when(k >= 2)
        def _():
            relay(0, k - 2)

    lead, lag, counts = SCHEDULE

    def step(k):
        chunk(1, k)
        if isinstance(k, int):
            if k >= lag:
                relay(1, k - lag)
        else:
            @pl.when(k >= lag)
            def _():
                relay(1, k - lag)

    for k in range(lead):
        step(k)
        if k >= lead - 2:
            relay(0, n_chunk - lead + k)

    squares(0, 0, n_chunk)
    normed(0)
    first_pair(0)
    each = counts[0] + counts[1]

    @pl.loop(0, 3)
    def _(j):
        for h in range(2):
            for c in range(counts[h]):
                step(lead + each * j + h * counts[0] + c)
            pair(0, 2 * j + 1 + h)

    k = lead + 3 * each
    rest = [lambda: last_pair(0), lambda: wait_heads(0), lambda: project(0, (0, 1, 2), False),
            lambda: project(0, (3, 4, 5), False), lambda: project(0, (6,), False)]
    done = k - lag
    for job in rest:
        if k < n_chunk:
            step(k)
            done = k - lag + 1
            k += 1
        elif done < n_chunk - 2:
            relay(1, done)
            done += 1
        job()
    while k < n_chunk:
        step(k)
        done = k - lag + 1
        k += 1

    @pl.loop(0, n_chunk)
    def _(k):
        for buf, s, r in ((obx, dx_s, dx_r), (obo, do_s, do_r)):
            mine = half_of(buf, k, core)
            remote(mine, mine, s.at[k], r.at[k], to_sib).wait_send()
        for p in range(2):
            send_part(p, k).wait_send()
        send_y(0, k).wait_send()
        relay_copy(0, k).wait_send()

    while done < n_chunk - 2:
        relay(1, done)
        done += 1
    squares(1, 0, n_chunk - 2)
    relay(1, n_chunk - 2)
    relay(1, n_chunk - 1)
    squares(1, n_chunk - 2, n_chunk)
    normed(1)
    first_pair(1)

    @pl.loop(1, n_pair)
    def _(i):
        pair(1, i)

    last_pair(1)
    drain_z(0)
    project_own(1, (0, 1, 2))

    @pl.loop(0, n_chunk)
    def _(k):
        send_y(1, k).wait_send()
        relay_copy(1, k).wait_send()

    wait_heads(1)
    project(1, (0, 1, 2), True)
    project(1, (3, 4, 5), False)
    project(1, (6,), False)
    drain_z(1)


def fused_block(stages, expert_out, expert_ids, slot_ids, gate_vals, residual, norm_w, w_query, w_key, w_value, w_out):
    n_exp, cap, d_model = expert_out.shape
    tokens = residual.shape[0]
    n_head, _, head_dim = w_query.shape
    width = 2 * head_dim
    n_chunk = d_model // width
    n_pair = n_head // 4
    size = [tokens * p // sum(PARTS) for p in PARTS]
    n_rows = 2 * n_exp * (cap // 4)
    n_pick = expert_ids.shape[0]
    dma = pltpu.SemaphoreType.DMA
    any_spec = pl.BlockSpec(memory_space=pl.ANY)
    vmem_spec = pl.BlockSpec(memory_space=pltpu.VMEM)
    vm = pltpu.VMEM

    def per_part(make):
        return [make(n) for n in size]

    return pl.pallas_call(
        functools.partial(fused_kernel, stages),
        out_shape=jax.ShapeDtypeStruct((tokens, d_model), BF16),
        in_specs=[any_spec, vmem_spec, vmem_spec, vmem_spec, any_spec, vmem_spec] + [any_spec] * 4,
        out_specs=any_spec,
        scratch_shapes=[
            vm((n_chunk, 2 * n_exp, cap // 4, width), BF16),
            vm((n_chunk, 2 * n_exp, cap // 4, width), BF16),
            vm((n_pick, tokens), jnp.int32),
            vm((n_pick, tokens), jnp.int32),
            vm((n_pick, tokens), F32),
            vm((3 * tokens, n_rows), BF16),
            vm((tokens, width), F32),
            vm((tokens, d_model), BF16),
            vm((tokens, width), BF16),
            vm((2, n_pair, tokens, width), BF16),
            vm((2, n_pair, tokens, width), BF16),
            vm((3, d_model, 3 * width), BF16),
        ] + per_part(lambda n: vm((n_chunk, n, width), F32)) * 2
          + per_part(lambda n: vm((n_chunk, n, width), F32))[1:]
          + per_part(lambda n: vm((n_chunk, n, width), BF16))
          + per_part(lambda n: vm((n_chunk, 2 * n, width), BF16))
          + per_part(lambda n: vm((2 * n, d_model), BF16))
          + [vm((n_pair, 2 * max(size), width), BF16)]
          + [dma((3,)), dma((3,)), dma((2,))]
          + [dma((n_chunk,))] * 6 + [dma((2 * n_chunk,))] * 6 + [dma((2 * n_pair,))] * 5 + [dma((3, 3))],
        compiler_params=pltpu.CompilerParams(collective_id=0, has_side_effects=True, vmem_limit_bytes=67_000_000),
        name='fused_block',
    )(expert_out, expert_ids, slot_ids, gate_vals, residual, norm_w, w_query, w_key, w_value, w_out)


def solution(mesh):
    stages = mesh.shape['pp']
    tok_spec = P('pp', 'ep', None, None)
    wt_spec = P('pp', None, None, None)

    def device_step(expert_out, expert_ids, slot_ids, gate_vals, residual, norm_w, w_query, w_key, w_value, w_out):
        heads = [w[0].transpose(1, 0, 2) for w in (w_query, w_key, w_value)]
        proj = w_out[0].reshape(-1, w_out.shape[3])
        result = fused_block(stages, expert_out[0], expert_ids[0, 0].T, slot_ids[0, 0].T, gate_vals[0, 0].T,
                             residual[0, 0], norm_w, *heads, proj)
        return result.reshape(residual.shape)

    return jax.shard_map(device_step, mesh=mesh, in_specs=(tok_spec, tok_spec, tok_spec, tok_spec, tok_spec, P('pp', None), wt_spec, wt_spec, wt_spec, wt_spec), out_specs=tok_spec, check_vma=False)
```
